32 devices in a mesh: rows: 4 (over z), feat: 8 (over y, x, core).
Axes of the slice: x: 2, y: 2, z: 4, core: 2. Of those that a mesh axis runs over, the one named last changes fastest.
Arguments:
- codes: int32 [65536, 512], P(('rows', 'feat')), may hold values from 0 to 255, as said below
- node_ids: int32 [2, 65536], P(None, ('rows', 'feat')), may hold values from 0 to 3
- bag_counts: int32 [2, 65536], P(None, ('rows', 'feat')), may hold values from 0 to 3
- labels: int32 [65536], P(('rows', 'feat')), may hold values from 0 to 1
Outputs:
- feature_gain: float32 [2, 4, 512], P(None, None, 'feat')
- node_gain: float32 [2, 4], replicated
The draws below stay inside these ranges and needn't reach their ends.
Inputs may be any that keep to these rules, and one draw needn't show every extreme that they name: Each feature's codes lie below a cap of that feature; bins above the cap are empty.
All inputs are finite; a program needn't handle non-finite values.
Results may differ from the reference program's by a relative error of at most 0.0003.
Values sent between devices are 32-bit elements; how exact they have to be, the bound alone decides.
A program may use at most 64 MiB of HBM per device.

```python
import math
import jax
import jax.numpy as jnp
import numpy as np
from jax import lax

F = 512
BINS = 256
CLASSES = 2
TREES = 2
NODES = 4
ROWS = 65536


def draw_codes(key, part):
    first_key, second_key = jax.random.split(jax.random.fold_in(key, 11))
    raw_codes = jax.random.randint(first_key, (ROWS, F), 0, BINS, dtype=jnp.int32)
    caps = jax.random.randint(second_key, (F,), BINS // 2, BINS, dtype=jnp.int32)
    return jnp.minimum(raw_codes, caps[None, :])


def set_ends(array, key, smallest, top_value):
    longest = array.shape.index(max(array.shape))
    spots = []
    for shift in (0, 1):
        where = [jax.random.randint(jax.random.fold_in(key, axis), (), 0, length) for axis, length in enumerate(array.shape)]
        where[longest] = (where[longest] + shift) % array.shape[longest]
        spots.append(tuple(where))
    return array.at[spots[0]].set(smallest).at[spots[1]].set(top_value)


def rank_table(amount, skew):
    weights = [(1 << 20) // math.isqrt(grade ** skew) + 1 for grade in range(1, amount + 1)]
    deviation = 1 + sum(weights) // (1 << 30)
    return np.cumsum(np.array([max(1, weight // deviation) for weight in weights]))


def ranked(rng, extent, count, skew):
    grid = rank_table(count, skew)
    pick = jax.random.randint(jax.random.fold_in(rng, 1), extent, 0, int(grid[count - 1]))
    standing = jnp.searchsorted(jnp.asarray(grid, jnp.int32), pick, side="right")
    return jax.random.permutation(jax.random.fold_in(rng, 2), count)[standing].astype(jnp.int32)


def setup_inputs(seed: int = 0) -> dict:
    arg_keys = jax.random.split(jax.random.key(seed), 5)
    return {
        "codes": draw_codes(jax.random.fold_in(arg_keys[4], 71), 0),
        "node_ids": set_ends(ranked(arg_keys[1], (TREES, ROWS), NODES, 2), jax.random.fold_in(arg_keys[1], 3), 0, NODES - 1).astype(jnp.int32),
        "bag_counts": set_ends(jax.random.randint(arg_keys[2], (TREES, ROWS), 0, 4), jax.random.fold_in(arg_keys[2], 1), 0, 3).astype(jnp.int32),
        "labels": set_ends(jax.random.randint(arg_keys[3], (ROWS,), 0, CLASSES), jax.random.fold_in(arg_keys[3], 1), 0, CLASSES - 1).astype(jnp.int32),
    }


def make_weights(node_ids, bag_counts, labels):
    node_range = jnp.arange(NODES, dtype=jnp.int32)
    class_range = jnp.arange(CLASSES, dtype=jnp.int32)
    node_hit = (node_ids[:, :, None] == node_range).astype(jnp.float32)
    class_hit = (labels[:, None] == class_range).astype(jnp.float32)
    weights = bag_counts.astype(jnp.float32)[:, :, None, None] * node_hit[:, :, :, None] * class_hit[None, :, None, :]
    count_rows = labels.shape[0]
    return jnp.transpose(weights, (1, 0, 2, 3)).reshape(count_rows, TREES * NODES * CLASSES)


def split_gains(left):
    feats = left.shape[0]
    left = left.reshape(feats, TREES, NODES, CLASSES, left.shape[-1])
    total = left[..., -1:]
    n_left = jnp.sum(left, axis=3, keepdims=True)
    n_total = jnp.sum(total, axis=3, keepdims=True)
    n_right = n_total - n_left
    frac = n_left / jnp.maximum(n_total, 1.0)
    spread_terms = (left - total * frac) ** 2
    scaled = n_total / (jnp.maximum(n_left, 1.0) * jnp.maximum(n_right, 1.0))
    spread = jnp.sum(spread_terms * scaled, axis=3)
    best = jnp.max(spread, axis=-1)
    return jnp.transpose(best, (1, 2, 0))


def reference(codes, node_ids, bag_counts, labels):
    weights = make_weights(node_ids, bag_counts, labels).astype(jnp.bfloat16).astype(jnp.float32)

    def one_feature(column):
        summed = jax.ops.segment_sum(weights, column.astype(jnp.int32), num_segments=BINS)
        return jnp.transpose(summed)

    hist = lax.map(one_feature, jnp.transpose(codes))
    left = jnp.cumsum(hist, axis=2)
    feature_gain = split_gains(left)
    node_gain = jnp.max(feature_gain, axis=2)
    return feature_gain, node_gain
```

```python
import functools
import math

import jax
import jax.numpy as jnp
from jax import lax
from jax.experimental import pallas as pl
from jax.experimental.pallas import tpu as pltpu
from jax.sharding import PartitionSpec as P

BINS = 256
CLASSES = 2
TREES = 2
NODES = 4
TN = TREES * NODES
LOW = 64
HIGH = BINS // LOW
PACK = 4096.0
CHUNK = 1024
GROUP = 4
MESH = pl.DeviceIdType.MESH


def plan(rows, feat, features):
    chips = feat // 2
    xs = 1 << (int(math.log2(chips)) // 2)
    ys = chips // xs
    local = features // feat
    rounds = 2 if local % (2 * 2 * GROUP) == 0 and local % (2 * 2 * rows) == 0 else 1
    return chips, xs, ys, local, rounds


def kernel(rows, feat, features, count_rows, ct_ref, meta_ref, fg_ref, node_ref,
           ct_in, meta_in, hi_ref, lo_ref, w_ref, sbuf, rbuf, zbuf, zup, zdown, gbuf, mbuf, min_ref,
           core_s, core_r, xy_s, xy_r, up_s, up_r, down_s, down_r, g_s, g_r, m_s, m_r):
    chips, xs, ys, local, rounds = plan(rows, feat, features)
    half = local // rounds // 2
    pairs = half // 2
    zb = half * 2 // rows // 2
    me = lax.axis_index("feat")
    z = lax.axis_index("rows")
    core = lax.rem(me, 2)
    chip = lax.div(me, 2)
    x = lax.rem(chip, xs)
    y = lax.div(chip, xs)

    def dev(yy, xx):
        return {"feat": (yy * xs + xx) * 2 + core}

    def feat_peer(k):
        return {"feat": lax.rem(me + k, feat)}

    def row_peer(k):
        return {"rows": lax.rem(z + k, rows)}

    barrier = pltpu.get_barrier_semaphore()
    for k in range(1, feat):
        pl.semaphore_signal(barrier, inc=1, device_id=feat_peer(k), device_id_type=MESH)
    for k in range(1, rows):
        pl.semaphore_signal(barrier, inc=1, device_id=row_peer(k), device_id_type=MESH)
    pl.semaphore_wait(barrier, feat - 1 + rows - 1)

    partner = {"feat": chip * 2 + 1 - core}
    pending = []

    def send(src, dst, s, r, device):
        copy = pltpu.make_async_remote_copy(
            src_ref=src, dst_ref=dst, send_sem=s, recv_sem=r, device_id=device, device_id_type=MESH)
        copy.start()
        pending.append(copy)
        return copy

    swaps = [send(meta_ref, meta_in, core_s.at[chips], core_r.at[chips], partner)]
    for q in range(chips):
        start = pl.multiple_of((2 * q + 1 - core) * local, local)
        swaps.append(send(ct_ref.at[pl.ds(start, local)], ct_in.at[pl.ds(q * local, local)],
                          core_s.at[q], core_r.at[q], partner))

    def weights(meta, base):
        row = lax.broadcasted_iota(jnp.int32, (TN, CHUNK), 0)
        tree = lax.div(row, NODES)
        node = lax.rem(row, NODES).astype(jnp.float32)

        def body(i, _):
            at = pl.ds(pl.multiple_of(i * CHUNK, CHUNK), CHUNK)
            m = meta[:, at]
            ids = jnp.where(tree == 0, m[0:1], m[1:2])
            bags = jnp.where(tree == 0, m[2:3], m[3:4])
            w = jnp.where(ids == node, bags * (1.0 + (PACK - 1.0) * m[4:5]), 0.0)
            out = pl.ds(pl.multiple_of(base + i * CHUNK, CHUNK), CHUNK)
            w_ref[:, out] = jnp.concatenate([w] * HIGH, axis=0).astype(jnp.bfloat16)
            return 0

        lax.fori_loop(0, count_rows // CHUNK, body, 0)

    def split(src, start, q, base):
        def body(i, _):
            code = src[pl.ds(pl.multiple_of(start + i * 8, 8), 8), :]
            high = jnp.floor(code * (1.0 / LOW))
            at = pl.ds(pl.multiple_of(q * local + i * 8, 8), 8)
            hi_ref[at, base:base + count_rows] = high
            lo_ref[at, base:base + count_rows] = code - LOW * high
            return 0

        lax.fori_loop(0, local // 8, body, 0)

    weights(meta_ref, 0)
    for q in range(chips):
        split(ct_ref, pl.multiple_of((2 * q + core) * local, local), q, 0)
    swaps[0].wait_recv()
    weights(meta_in, count_rows)
    for q in range(chips):
        swaps[1 + q].wait_recv()
        split(ct_in, q * local, q, count_rows)

    hi_of = lax.div(lax.broadcasted_iota(jnp.int32, (HIGH * TN, CHUNK), 0), TN).astype(jnp.float32).astype(jnp.bfloat16)
    lo_of = lax.broadcasted_iota(jnp.int32, (LOW, CHUNK), 0).astype(jnp.float32).astype(jnp.bfloat16)
    one = jnp.ones((), jnp.bfloat16)
    zero = jnp.zeros((), jnp.bfloat16)
    first_half = lax.broadcasted_iota(jnp.int32, (HIGH * TN, 2 * LOW), 1) < LOW

    def compute(out, owner, offset, adds):
        first = owner * local + offset

        def body(g, _):
            f0 = first + g * GROUP
            low_sum = [None] * (GROUP // 2)
            high_sum = [None] * (GROUP // 2)
            for c in range(2 * count_rows // CHUNK):
                at = slice(c * CHUNK, (c + 1) * CHUNK)
                w = w_ref[:, at]
                a, b = [], []
                for k in range(GROUP):
                    high = jnp.broadcast_to(hi_ref[pl.ds(f0 + k, 1), at], (HIGH * TN, CHUNK)).astype(jnp.bfloat16)
                    low = jnp.broadcast_to(lo_ref[pl.ds(f0 + k, 1), at], (LOW, CHUNK)).astype(jnp.bfloat16)
                    a.append(jnp.where(high == hi_of, w, zero))
                    b.append(jnp.where(low == lo_of, one, zero))
                r = lax.dot_general(jnp.concatenate(a, axis=0), jnp.concatenate(b, axis=0),
                                    (((1,), (1,)), ((), ())), preferred_element_type=jnp.float32)
                size = HIGH * TN
                for p in range(GROUP // 2):
                    cols = slice(2 * LOW * p, 2 * LOW * (p + 1))
                    v = jnp.where(first_half, r[2 * p * size:(2 * p + 1) * size, cols],
                                  r[(2 * p + 1) * size:(2 * p + 2) * size, cols])
                    top = jnp.floor(v * (1.0 / PACK))
                    rest = v - PACK * top
                    low_sum[p] = rest if c == 0 else low_sum[p] + rest
                    high_sum[p] = top if c == 0 else high_sum[p] + top
            for p in range(GROUP // 2):
                slot = g * (GROUP // 2) + p
                value = jnp.concatenate([low_sum[p], high_sum[p]], axis=0)
                for add in adds:
                    value = value + add[slot]
                out[slot] = value
            return 0

        lax.fori_loop(0, half // GROUP, body, 0)

    n1a = (xs - 1) * ys
    n1b = (ys - 1) * xs
    slots = n1a + n1b + (ys - 1) + (xs - 1)

    def xy_round(rd):
        base = rd * slots
        offa = rd * 2 * half
        offb = offa + half
        copies = {}

        def go(slot, device):
            s = base + slot
            copies[slot] = send(sbuf.at[s], rbuf.at[s], xy_s.at[s], xy_r.at[s], device)

        def a_slot(dx, dy):
            return (dx - 1) * ys + dy

        def b_slot(dy, dx):
            return n1a + (dy - 1) * xs + dx

        def c_slot(dy):
            return n1a + n1b + dy - 1

        def d_slot(dx):
            return n1a + n1b + ys - 1 + dx - 1

        units = []

        def unit_a(dx, dy):
            xx, yy = lax.rem(x + dx, xs), lax.rem(y + dy, ys)
            s = a_slot(dx, dy)
            compute(sbuf.at[base + s], yy * xs + xx, offa, [])
            go(s, dev(y, xx))

        def unit_b(dy, dx):
            xx, yy = lax.rem(x + dx, xs), lax.rem(y + dy, ys)
            s = b_slot(dy, dx)
            compute(sbuf.at[base + s], yy * xs + xx, offb, [])
            go(s, dev(yy, x))

        def landed(s):
            copies[s].wait_recv()
            return rbuf.at[base + s]

        def unit_c(dy):
            yy = lax.rem(y + dy, ys)
            s = c_slot(dy)
            adds = [landed(a_slot(dx, dy)) for dx in range(1, xs)]
            compute(sbuf.at[base + s], yy * xs + x, offa, adds)
            go(s, dev(yy, x))

        def unit_d(dx):
            xx = lax.rem(x + dx, xs)
            s = d_slot(dx)
            adds = [landed(b_slot(dy, dx)) for dy in range(1, ys)]
            compute(sbuf.at[base + s], y * xs + xx, offb, adds)
            go(s, dev(y, xx))

        def own(which):
            if which == 0:
                near = [landed(a_slot(dx, 0)) for dx in range(1, xs)]
            else:
                near = [landed(b_slot(dy, 0)) for dy in range(1, ys)]
            compute(zbuf.at[rd, pl.ds(which * pairs, pairs)], chip, offb if which else offa, near)

        def own_late(which):
            far = [landed(c_slot(dy)) for dy in range(1, ys)] if which == 0 else [landed(d_slot(dx)) for dx in range(1, xs)]

            def body(i, _):
                value = zbuf[rd, which * pairs + i]
                for ref in far:
                    value = value + ref[i]
                zbuf[rd, which * pairs + i] = value
                return 0

            lax.fori_loop(0, pairs, body, 0)

        stage_a = [functools.partial(unit_a, dx, dy) for dy in range(ys - 1, -1, -1) for dx in range(1, xs)]
        stage_b = [functools.partial(unit_b, dy, dx) for dx in range(xs - 1, -1, -1) for dy in range(1, ys)]
        for i in range(max(len(stage_a), len(stage_b))):
            units += stage_a[i:i + 1] + stage_b[i:i + 1]
        stage_c = [functools.partial(unit_c, dy) for dy in range(1, ys)]
        stage_d = [functools.partial(unit_d, dx) for dx in range(1, xs)]
        for i in range(max(len(stage_c), len(stage_d))):
            units += stage_c[i:i + 1] + stage_d[i:i + 1]
        units += [functools.partial(own, 0), functools.partial(own, 1)]
        lates = [functools.partial(own_late, 0), functools.partial(own_late, 1)]
        return units, lates

    def add_block(rd, j, ref):
        def body(i, _):
            zbuf[rd, j * zb + i] = zbuf[rd, j * zb + i] + ref[rd, j, i]
            return 0

        lax.fori_loop(0, zb, body, 0)

    def up_copy(rd, j):
        return pltpu.make_async_remote_copy(
            src_ref=zbuf.at[rd, pl.ds(j * zb, zb)], dst_ref=zup.at[rd, j],
            send_sem=up_s.at[rd * rows + j], recv_sem=up_r.at[rd * rows + j],
            device_id=row_peer(1), device_id_type=MESH)

    def down_copy(rd, j):
        return pltpu.make_async_remote_copy(
            src_ref=zbuf.at[rd, pl.ds(j * zb, zb)], dst_ref=zdown.at[rd, j],
            send_sem=down_s.at[rd * rows + j], recv_sem=down_r.at[rd * rows + j],
            device_id=row_peer(rows - 1), device_id_type=MESH)

    def z_part(rd, i):
        j = rows - 1 - i

        @pl.when(z <= j)
        def _():
            @pl.when(z > 0)
            def _():
                up_copy(rd, j).wait_recv()
                add_block(rd, j, zup)

            @pl.when(z < j)
            def _():
                up_copy(rd, j).start()

        @pl.when(z >= i)
        def _():
            @pl.when(z < rows - 1)
            def _():
                down_copy(rd, i).wait_recv()
                add_block(rd, i, zdown)

            @pl.when(z > i)
            def _():
                down_copy(rd, i).start()

    def z_sent(rd):
        for j in range(rows):
            @pl.when(z < j)
            def _():
                up_copy(rd, j).wait_send()

            @pl.when(z > j)
            def _():
                down_copy(rd, j).wait_send()

    lane_r = lax.broadcasted_iota(jnp.int32, (2 * LOW, 2 * LOW), 0)
    lane_c = lax.broadcasted_iota(jnp.int32, (2 * LOW, 2 * LOW), 1)
    same = lax.div(lane_r, LOW) == lax.div(lane_c, LOW)
    upper = jnp.where(same & (lane_r <= lane_c), 1.0, 0.0)
    whole = jnp.where(same, 1.0, 0.0)
    left_lanes = lax.broadcasted_iota(jnp.int32, (TN, 2 * LOW), 1) < LOW

    def gains(rd):
        def body(i, _):
            h = zbuf[rd, z * zb + i]
            inner = jnp.dot(h, upper, precision=lax.Precision.HIGHEST, preferred_element_type=jnp.float32)
            sums = jnp.dot(h, whole, precision=lax.Precision.HIGHEST, preferred_element_type=jnp.float32)
            left = [[None] * HIGH for _ in range(CLASSES)]
            total = []
            for c in range(CLASSES):
                carry = jnp.zeros((TN, 2 * LOW), jnp.float32)
                for k in range(HIGH):
                    at = (c * HIGH + k) * TN
                    left[c][k] = inner[at:at + TN] + carry
                    carry = carry + sums[at:at + TN]
                total.append(carry)
            n_total = total[0] + total[1]
            safe = jnp.maximum(n_total, 1.0)
            best = None
            for k in range(HIGH):
                n_left = left[0][k] + left[1][k]
                n_right = n_total - n_left
                frac = n_left / safe
                scaled = n_total / (jnp.maximum(n_left, 1.0) * jnp.maximum(n_right, 1.0))
                spread = (left[0][k] - total[0] * frac) ** 2 * scaled + (left[1][k] - total[1] * frac) ** 2 * scaled
                best = spread if best is None else jnp.maximum(best, spread)
            even = jnp.max(jnp.where(left_lanes, best, 0.0), axis=1, keepdims=True)
            odd = jnp.max(jnp.where(left_lanes, 0.0, best), axis=1, keepdims=True)
            gbuf[0, rd * zb + i] = jnp.where(left_lanes, even, odd)
            return 0

        lax.fori_loop(0, zb, body, 0)

    previous = None
    for rd in range(rounds):
        units, lates = xy_round(rd)
        parts = [] if previous is None else [functools.partial(z_part, previous, i) for i in range(rows)]
        every = max(1, len(units) // (len(parts) + 1))
        for n, unit in enumerate(units):
            unit()
            if parts and (n + 1) % every == 0:
                parts.pop(0)()
        for part in parts:
            part()
        if previous is not None:
            gains(previous)
        for late in lates:
            late()
        previous = rd
    for i in range(rows):
        z_part(previous, i)
    gains(previous)

    size = rounds * zb
    copies = [send(gbuf.at[0], gbuf.at[k], g_s.at[k], g_r.at[k], row_peer(k)) for k in range(1, rows)]
    for copy in copies:
        copy.wait_recv()
    top = None
    for k in range(rows):
        origin = lax.rem(z - k + rows, rows)
        for rd in range(rounds):
            for i in range(zb):
                value = gbuf[k, rd * zb + i]
                fg_ref[rd * rows * zb + origin * zb + i] = value
                top = value if top is None else jnp.maximum(top, value)
    mbuf[...] = jnp.broadcast_to(jnp.max(top, axis=1, keepdims=True), (TN, 2 * LOW))
    copies = [send(mbuf, min_ref.at[k], m_s.at[k], m_r.at[k], feat_peer(k)) for k in range(1, feat)]
    best = mbuf[...]
    for k in range(1, feat):
        copies[k - 1].wait_recv()
        best = jnp.maximum(best, min_ref[k])
    node_ref[...] = best
    for copy in pending:
        copy.wait_send()
    for rd in range(rounds):
        z_sent(rd)


def on_device(rows, feat, codes, node_ids, bag_counts, labels):
    count_rows, features = codes.shape
    chips, xs, ys, local, rounds = plan(rows, feat, features)
    half = local // rounds // 2
    pairs = half // 2
    zb = half * 2 // rows // 2
    slots = (xs - 1) * ys + (ys - 1) * xs + (ys - 1) + (xs - 1)
    tile = (CLASSES * HIGH * TN, 2 * LOW)
    ct = jnp.transpose(codes).astype(jnp.float32)
    meta = jnp.concatenate([node_ids, bag_counts, labels[None], jnp.zeros((3, count_rows), jnp.int32)], axis=0).astype(jnp.float32)
    vmem = pl.BlockSpec(memory_space=pltpu.VMEM)
    dma = lambda n: pltpu.SemaphoreType.DMA((n,))
    f32 = jnp.float32
    fg, node = pl.pallas_call(
        functools.partial(kernel, rows, feat, features, count_rows),
        out_shape=(jax.ShapeDtypeStruct((local // 2, TN, 2 * LOW), f32), jax.ShapeDtypeStruct((TN, 2 * LOW), f32)),
        in_specs=[vmem, vmem],
        out_specs=(vmem, vmem),
        scratch_shapes=[
            pltpu.VMEM((features // 2, count_rows), f32),
            pltpu.VMEM(meta.shape, f32),
            pltpu.VMEM((features // 2, 2 * count_rows), f32),
            pltpu.VMEM((features // 2, 2 * count_rows), f32),
            pltpu.VMEM((HIGH * TN, 2 * count_rows), jnp.bfloat16),
            pltpu.VMEM((rounds * slots, pairs) + tile, f32),
            pltpu.VMEM((rounds * slots, pairs) + tile, f32),
            pltpu.VMEM((rounds, 2 * pairs) + tile, f32),
            pltpu.VMEM((rounds, rows, zb) + tile, f32),
            pltpu.VMEM((rounds, rows, zb) + tile, f32),
            pltpu.VMEM((rows, rounds * zb, TN, 2 * LOW), f32),
            pltpu.VMEM((TN, 2 * LOW), f32),
            pltpu.VMEM((feat, TN, 2 * LOW), f32),
            dma(chips + 1), dma(chips + 1),
            dma(rounds * slots), dma(rounds * slots),
            dma(rounds * rows), dma(rounds * rows), dma(rounds * rows), dma(rounds * rows),
            dma(rows), dma(rows), dma(feat), dma(feat),
        ],
        compiler_params=pltpu.CompilerParams(
            collective_id=0, has_side_effects=True, vmem_limit_bytes=60 * 1024 * 1024),
    )(ct, meta)
    both = jnp.stack([fg[:, :, 0], fg[:, :, LOW]], axis=1)
    feature_gain = jnp.transpose(both.reshape(local, TN)).reshape(TREES, NODES, local)
    return feature_gain, node[:, 0].reshape(TREES, NODES)


def solution(mesh):
    return jax.shard_map(
        functools.partial(on_device, mesh.shape["rows"], mesh.shape["feat"]),
        mesh=mesh,
        in_specs=(
            P(("rows", "feat"), None),
            P(None, ("rows", "feat")),
            P(None, ("rows", "feat")),
            P(("rows", "feat")),
        ),
        out_specs=(P(None, None, "feat"), P()),
        check_vma=False,
    )
```

```python
import functools
import math

import jax
import jax.numpy as jnp
from jax import lax
from jax.experimental import pallas as pl
from jax.experimental.pallas import tpu as pltpu
from jax.sharding import PartitionSpec as P

BINS = 256
CLASSES = 2
TREES = 2
NODES = 4
TN = TREES * NODES
LOW = 64
HIGH = BINS // LOW
PACK = 4096.0
CHUNK = 1024
GROUP = 4
MESH = pl.DeviceIdType.MESH


def plan(rows, feat, features):
    chips = feat // 2
    xs = 1 << (int(math.log2(chips)) // 2)
    ys = chips // xs
    local = features // feat
    rounds = 2 if local % (2 * 2 * GROUP) == 0 and local % (2 * 2 * rows) == 0 else 1
    return chips, xs, ys, local, rounds


def kernel(rows, feat, features, count_rows, ct_ref, meta_ref, fg_ref, node_ref,
           ct_in, meta_in, hi_ref, lo_ref, w_ref, sbuf, rbuf, zbuf, zin, gbuf, mbuf, min_ref,
           core_s, core_r, xy_s, xy_r, z_s, z_r, g_s, g_r, m_s, m_r):
    chips, xs, ys, local, rounds = plan(rows, feat, features)
    half = local // rounds // 2
    pairs = half // 2
    zb = half * 2 // rows // 2
    me = lax.axis_index("feat")
    z = lax.axis_index("rows")
    core = lax.rem(me, 2)
    chip = lax.div(me, 2)
    x = lax.rem(chip, xs)
    y = lax.div(chip, xs)

    def dev(yy, xx):
        return {"feat": (yy * xs + xx) * 2 + core}

    def feat_peer(k):
        return {"feat": lax.rem(me + k, feat)}

    def row_peer(k):
        return {"rows": lax.rem(z + k, rows)}

    barrier = pltpu.get_barrier_semaphore()
    for k in range(1, feat):
        pl.semaphore_signal(barrier, inc=1, device_id=feat_peer(k), device_id_type=MESH)
    for k in range(1, rows):
        pl.semaphore_signal(barrier, inc=1, device_id=row_peer(k), device_id_type=MESH)
    pl.semaphore_wait(barrier, feat - 1 + rows - 1)

    partner = {"feat": chip * 2 + 1 - core}
    pending = []

    def send(src, dst, s, r, device):
        copy = pltpu.make_async_remote_copy(
            src_ref=src, dst_ref=dst, send_sem=s, recv_sem=r, device_id=device, device_id_type=MESH)
        copy.start()
        pending.append(copy)
        return copy

    swaps = [send(meta_ref, meta_in, core_s.at[chips], core_r.at[chips], partner)]
    for q in range(chips):
        start = pl.multiple_of((2 * q + 1 - core) * local, local)
        swaps.append(send(ct_ref.at[pl.ds(start, local)], ct_in.at[pl.ds(q * local, local)],
                          core_s.at[q], core_r.at[q], partner))

    def weights(meta, base):
        row = lax.broadcasted_iota(jnp.int32, (TN, CHUNK), 0)
        tree = lax.div(row, NODES)
        node = lax.rem(row, NODES).astype(jnp.float32)

        def body(i, _):
            at = pl.ds(pl.multiple_of(i * CHUNK, CHUNK), CHUNK)
            m = meta[:, at]
            ids = jnp.where(tree == 0, m[0:1], m[1:2])
            bags = jnp.where(tree == 0, m[2:3], m[3:4])
            w = jnp.where(ids == node, bags * (1.0 + (PACK - 1.0) * m[4:5]), 0.0)
            out = pl.ds(pl.multiple_of(base + i * CHUNK, CHUNK), CHUNK)
            w_ref[:, out] = jnp.concatenate([w] * HIGH, axis=0).astype(jnp.bfloat16)
            return 0

        lax.fori_loop(0, count_rows // CHUNK, body, 0)

    def split(src, start, q, base):
        def body(i, _):
            code = src[pl.ds(pl.multiple_of(start + i * 8, 8), 8), :]
            high = lax.shift_right_logical(code, LOW.bit_length() - 1)
            at = pl.ds(pl.multiple_of(q * local + i * 8, 8), 8)
            hi_ref[at, base:base + count_rows] = high.astype(jnp.float32)
            lo_ref[at, base:base + count_rows] = (code & (LOW - 1)).astype(jnp.float32)
            return 0

        lax.fori_loop(0, local // 8, body, 0)

    weights(meta_ref, 0)
    for q in range(chips):
        split(ct_ref, pl.multiple_of((2 * q + core) * local, local), q, 0)
    swaps[0].wait_recv()
    weights(meta_in, count_rows)
    for q in range(chips):
        swaps[1 + q].wait_recv()
        split(ct_in, q * local, q, count_rows)

    hi_of = lax.div(lax.broadcasted_iota(jnp.int32, (HIGH * TN, CHUNK), 0), TN).astype(jnp.float32).astype(jnp.bfloat16)
    lo_of = lax.broadcasted_iota(jnp.int32, (LOW, CHUNK), 0).astype(jnp.float32).astype(jnp.bfloat16)
    one = jnp.ones((), jnp.bfloat16)
    zero = jnp.zeros((), jnp.bfloat16)
    first_half = lax.broadcasted_iota(jnp.int32, (HIGH * TN, 2 * LOW), 1) < LOW

    def compute(out, owner, offset, adds):
        first = owner * local + offset

        def body(g, _):
            f0 = first + g * GROUP
            low_sum = [None] * (GROUP // 2)
            high_sum = [None] * (GROUP // 2)
            for c in range(2 * count_rows // CHUNK):
                at = slice(c * CHUNK, (c + 1) * CHUNK)
                w = w_ref[:, at]
                a, b = [], []
                for k in range(GROUP):
                    high = jnp.broadcast_to(hi_ref[pl.ds(f0 + k, 1), at], (HIGH * TN, CHUNK)).astype(jnp.bfloat16)
                    low = jnp.broadcast_to(lo_ref[pl.ds(f0 + k, 1), at], (LOW, CHUNK)).astype(jnp.bfloat16)
                    a.append(jnp.where(high == hi_of, w, zero))
                    b.append(jnp.where(low == lo_of, one, zero))
                ones = jnp.concatenate(b, axis=0).astype(jnp.float8_e4m3fn)
                r = lax.dot_general(jnp.concatenate(a, axis=0), ones,
                                    (((1,), (1,)), ((), ())), preferred_element_type=jnp.float32)
                size = HIGH * TN
                for p in range(GROUP // 2):
                    cols = slice(2 * LOW * p, 2 * LOW * (p + 1))
                    v = jnp.where(first_half, r[2 * p * size:(2 * p + 1) * size, cols],
                                  r[(2 * p + 1) * size:(2 * p + 2) * size, cols])
                    top = jnp.floor(v * (1.0 / PACK))
                    rest = v - PACK * top
                    low_sum[p] = rest if c == 0 else low_sum[p] + rest
                    high_sum[p] = top if c == 0 else high_sum[p] + top
            for p in range(GROUP // 2):
                slot = g * (GROUP // 2) + p
                value = jnp.concatenate([low_sum[p], high_sum[p]], axis=0)
                for add in adds:
                    value = value + add[slot]
                out[slot] = value
            return 0

        lax.fori_loop(0, half // GROUP, body, 0)

    n1a = (xs - 1) * ys
    n1b = (ys - 1) * xs
    slots = n1a + n1b + (ys - 1) + (xs - 1)

    def xy_round(rd):
        base = rd * slots
        offa = rd * 2 * half
        offb = offa + half
        copies = {}

        def go(slot, device):
            s = base + slot
            copies[slot] = send(sbuf.at[s], rbuf.at[s], xy_s.at[s], xy_r.at[s], device)

        def a_slot(dx, dy):
            return (dx - 1) * ys + dy

        def b_slot(dy, dx):
            return n1a + (dy - 1) * xs + dx

        def c_slot(dy):
            return n1a + n1b + dy - 1

        def d_slot(dx):
            return n1a + n1b + ys - 1 + dx - 1

        units = []

        def unit_a(dx, dy):
            xx, yy = lax.rem(x + dx, xs), lax.rem(y + dy, ys)
            s = a_slot(dx, dy)
            compute(sbuf.at[base + s], yy * xs + xx, offa, [])
            go(s, dev(y, xx))

        def unit_b(dy, dx):
            xx, yy = lax.rem(x + dx, xs), lax.rem(y + dy, ys)
            s = b_slot(dy, dx)
            compute(sbuf.at[base + s], yy * xs + xx, offb, [])
            go(s, dev(yy, x))

        def landed(s):
            copies[s].wait_recv()
            return rbuf.at[base + s]

        def unit_c(dy):
            yy = lax.rem(y + dy, ys)
            s = c_slot(dy)
            adds = [landed(a_slot(dx, dy)) for dx in range(1, xs)]
            compute(sbuf.at[base + s], yy * xs + x, offa, adds)
            go(s, dev(yy, x))

        def unit_d(dx):
            xx = lax.rem(x + dx, xs)
            s = d_slot(dx)
            adds = [landed(b_slot(dy, dx)) for dy in range(1, ys)]
            compute(sbuf.at[base + s], y * xs + xx, offb, adds)
            go(s, dev(y, xx))

        def own(which):
            if which == 0:
                near = [landed(a_slot(dx, 0)) for dx in range(1, xs)]
            else:
                near = [landed(b_slot(dy, 0)) for dy in range(1, ys)]
            compute(zbuf.at[rd, pl.ds(which * pairs, pairs)], chip, offb if which else offa, near)

        def own_late(which):
            far = [landed(c_slot(dy)) for dy in range(1, ys)] if which == 0 else [landed(d_slot(dx)) for dx in range(1, xs)]

            def body(i, _):
                value = zbuf[rd, which * pairs + i]
                for ref in far:
                    value = value + ref[i]
                zbuf[rd, which * pairs + i] = value
                return 0

            lax.fori_loop(0, pairs, body, 0)

        stage_a = [functools.partial(unit_a, dx, dy) for dy in range(ys - 1, -1, -1) for dx in range(1, xs)]
        stage_b = [functools.partial(unit_b, dy, dx) for dx in range(xs - 1, -1, -1) for dy in range(1, ys)]
        for i in range(max(len(stage_a), len(stage_b))):
            units += stage_a[i:i + 1] + stage_b[i:i + 1]
        stage_c = [functools.partial(unit_c, dy) for dy in range(1, ys)]
        stage_d = [functools.partial(unit_d, dx) for dx in range(1, xs)]
        for i in range(max(len(stage_c), len(stage_d))):
            units += stage_c[i:i + 1] + stage_d[i:i + 1]
        units += [functools.partial(own, 0), functools.partial(own, 1)]
        lates = [functools.partial(own_late, 0), functools.partial(own_late, 1)]
        return units, lates

    def z_start(rd):
        for k in range(1, rows):
            j = lax.rem(z + k, rows)
            n = rd * rows + k
            zcopies[n] = send(zbuf.at[rd, pl.ds(j * zb, zb)], zin.at[rd, k], z_s.at[n], z_r.at[n], row_peer(k))

    def z_landed(rd):
        for k in range(1, rows):
            zcopies[rd * rows + k].wait_recv()

    zcopies = {}
    lane_r = lax.broadcasted_iota(jnp.int32, (2 * LOW, 2 * LOW), 0)
    lane_c = lax.broadcasted_iota(jnp.int32, (2 * LOW, 2 * LOW), 1)
    same = lax.div(lane_r, LOW) == lax.div(lane_c, LOW)
    upper = jnp.where(same & (lane_r <= lane_c), 1.0, 0.0)
    whole = jnp.where(same, 1.0, 0.0)
    left_lanes = lax.broadcasted_iota(jnp.int32, (TN, 2 * LOW), 1) < LOW

    def gains(rd):
        block = CLASSES * HIGH * TN
        h = zbuf[rd, pl.ds(z * zb, zb)]
        for k in range(1, rows):
            h = h + zin[rd, k]
        h = h.reshape(zb * block, 2 * LOW)
        inner_all = jnp.dot(h, upper, precision=lax.Precision.HIGHEST, preferred_element_type=jnp.float32)
        sums_all = jnp.dot(h, whole, precision=lax.Precision.HIGHEST, preferred_element_type=jnp.float32)
        for i in range(zb):
            inner = inner_all[i * block:(i + 1) * block]
            sums = sums_all[i * block:(i + 1) * block]
            left = [[None] * HIGH for _ in range(CLASSES)]
            total = []
            for c in range(CLASSES):
                carry = jnp.zeros((TN, 2 * LOW), jnp.float32)
                for k in range(HIGH):
                    at = (c * HIGH + k) * TN
                    left[c][k] = inner[at:at + TN] + carry
                    carry = carry + sums[at:at + TN]
                total.append(carry)
            n_total = total[0] + total[1]
            safe = jnp.maximum(n_total, 1.0)
            best = None
            for k in range(HIGH):
                n_left = left[0][k] + left[1][k]
                n_right = n_total - n_left
                frac = n_left / safe
                scaled = n_total / (jnp.maximum(n_left, 1.0) * jnp.maximum(n_right, 1.0))
                spread = (left[0][k] - total[0] * frac) ** 2 * scaled + (left[1][k] - total[1] * frac) ** 2 * scaled
                best = spread if best is None else jnp.maximum(best, spread)
            even = jnp.max(jnp.where(left_lanes, best, 0.0), axis=1, keepdims=True)
            odd = jnp.max(jnp.where(left_lanes, 0.0, best), axis=1, keepdims=True)
            gbuf[0, rd * zb + i] = jnp.where(left_lanes, even, odd)

    previous = None
    for rd in range(rounds):
        units, lates = xy_round(rd)
        for unit in units:
            unit()
        for late in lates:
            late()
        z_start(rd)
        if previous is not None:
            z_landed(previous)
            gains(previous)
        previous = rd
    z_landed(previous)
    gains(previous)

    copies = [send(gbuf.at[0], gbuf.at[k], g_s.at[k], g_r.at[k], row_peer(k)) for k in range(1, rows)]
    for copy in copies:
        copy.wait_recv()
    top = None
    for k in range(rows):
        origin = lax.rem(z - k + rows, rows)
        for rd in range(rounds):
            for i in range(zb):
                value = gbuf[k, rd * zb + i]
                fg_ref[rd * rows * zb + origin * zb + i] = value
                top = value if top is None else jnp.maximum(top, value)
    mbuf[...] = jnp.broadcast_to(jnp.max(top, axis=1, keepdims=True), (TN, 2 * LOW))
    copies = [send(mbuf, min_ref.at[k], m_s.at[k], m_r.at[k], feat_peer(k)) for k in range(1, feat)]
    best = mbuf[...]
    for k in range(1, feat):
        copies[k - 1].wait_recv()
        best = jnp.maximum(best, min_ref[k])
    node_ref[...] = best
    for copy in pending:
        copy.wait_send()


def on_device(rows, feat, codes, node_ids, bag_counts, labels):
    count_rows, features = codes.shape
    chips, xs, ys, local, rounds = plan(rows, feat, features)
    half = local // rounds // 2
    pairs = half // 2
    zb = half * 2 // rows // 2
    slots = (xs - 1) * ys + (ys - 1) * xs + (ys - 1) + (xs - 1)
    tile = (CLASSES * HIGH * TN, 2 * LOW)
    ct = jnp.transpose(codes)
    meta = jnp.concatenate([node_ids, bag_counts, labels[None], jnp.zeros((3, count_rows), jnp.int32)], axis=0).astype(jnp.float32)
    vmem = pl.BlockSpec(memory_space=pltpu.VMEM)
    dma = lambda n: pltpu.SemaphoreType.DMA((n,))
    f32 = jnp.float32
    fg, node = pl.pallas_call(
        functools.partial(kernel, rows, feat, features, count_rows),
        out_shape=(jax.ShapeDtypeStruct((local // 2, TN, 2 * LOW), f32), jax.ShapeDtypeStruct((TN, 2 * LOW), f32)),
        in_specs=[vmem, vmem],
        out_specs=(vmem, vmem),
        scratch_shapes=[
            pltpu.VMEM((features // 2, count_rows), jnp.int32),
            pltpu.VMEM(meta.shape, f32),
            pltpu.VMEM((features // 2, 2 * count_rows), f32),
            pltpu.VMEM((features // 2, 2 * count_rows), f32),
            pltpu.VMEM((HIGH * TN, 2 * count_rows), jnp.bfloat16),
            pltpu.VMEM((rounds * slots, pairs) + tile, f32),
            pltpu.VMEM((rounds * slots, pairs) + tile, f32),
            pltpu.VMEM((rounds, 2 * pairs) + tile, f32),
            pltpu.VMEM((rounds, rows, zb) + tile, f32),
            pltpu.VMEM((rows, rounds * zb, TN, 2 * LOW), f32),
            pltpu.VMEM((TN, 2 * LOW), f32),
            pltpu.VMEM((feat, TN, 2 * LOW), f32),
            dma(chips + 1), dma(chips + 1),
            dma(rounds * slots), dma(rounds * slots),
            dma(rounds * rows), dma(rounds * rows),
            dma(rows), dma(rows), dma(feat), dma(feat),
        ],
        compiler_params=pltpu.CompilerParams(
            collective_id=0, has_side_effects=True, vmem_limit_bytes=60 * 1024 * 1024),
    )(ct, meta)
    both = jnp.stack([fg[:, :, 0], fg[:, :, LOW]], axis=1)
    feature_gain = jnp.transpose(both.reshape(local, TN)).reshape(TREES, NODES, local)
    return feature_gain, node[:, 0].reshape(TREES, NODES)


def solution(mesh):
    return jax.shard_map(
        functools.partial(on_device, mesh.shape["rows"], mesh.shape["feat"]),
        mesh=mesh,
        in_specs=(
            P(("rows", "feat"), None),
            P(None, ("rows", "feat")),
            P(None, ("rows", "feat")),
            P(("rows", "feat")),
        ),
        out_specs=(P(None, None, "feat"), P()),
        check_vma=False,
    )
```
